128 devices in a mesh: dev: 128 (over x, y, z, core).
Axes of the slice: x: 4, y: 4, z: 4, core: 2. Of those that a mesh axis runs over, the one named last changes fastest.
Arguments:
- source: bfloat16 [48, 1048576], P(None, 'dev'), may hold values from -6 to 6
- weights: bfloat16 [81920, 128, 128], P('dev'), may hold values from -0.01953125 to 0.01953125
- tile_map: int32 [3, 81920], P(None, 'dev'), may hold values from 0 to 127, as said below
- tile_count: int32 [128], P('dev'), may hold values from 160 to 640, as said below
Outputs:
- acoustic_source: float32 [48, 16384], P(None, 'dev')
The draws below stay inside these ranges and needn't reach their ends.
Inputs may be any that keep to these rules, and one draw needn't show every extreme that they name: `tile_map`: row 0 is a CFD block of the owning device; row 2 an acoustic block of the destination. Row 1 is a device at cyclic distance at most 4 from the owner in device order, or at distance exactly 128 // 2 (counted upward); every device has used slots at distance +4, -4 and 128 // 2. `tile_count`: some device uses all its slots.
All inputs are finite; a program needn't handle non-finite values.
Results may differ from the reference program's by a relative error of at most 0.0003.
Values sent between devices are 32-bit elements; how exact they have to be, the bound alone decides.
A program may use at most 128 MiB of HBM per device.

```python
import jax
import jax.numpy as jnp
from jax import lax

BLK = 128
REACH = 4
SRC_BLK_DEV = 64
TILES_DEV = 640
ACU_BLK_DEV = 1
FEAT = 48
CELLS = 1048576
TILES = 81920
N_DEV = 128


def draw_tile_map(key, part):
    key_src = jax.random.fold_in(key, 11)
    key_off = jax.random.fold_in(key, 12)
    key_blk = jax.random.fold_in(key, 13)
    total = N_DEV * TILES_DEV
    src_ids = jax.random.randint(key_src, (total,), 0, SRC_BLK_DEV)
    offsets = jax.random.randint(key_off, (total,), -REACH, REACH + 1)
    slot = jnp.arange(total) % TILES_DEV
    offsets = jnp.where(slot == 0, REACH, jnp.where(slot == 1, -REACH, jnp.where(slot == 2, N_DEV // 2, offsets)))
    owner = jnp.arange(total) // TILES_DEV
    dest = (owner + offsets) % N_DEV
    dest_blk = jax.random.randint(key_blk, (total,), 0, ACU_BLK_DEV)
    return jnp.stack([src_ids, dest, dest_blk]).astype(jnp.int32)


def draw_tile_count(key, part):
    key_cnt = jax.random.fold_in(key, 21)
    key_full = jax.random.fold_in(key, 22)
    lowest = max(TILES_DEV // 4, 3)
    counts = jax.random.randint(key_cnt, (N_DEV,), lowest, TILES_DEV + 1)
    busiest = jax.random.randint(key_full, (), 0, N_DEV)
    counts = jnp.where(jnp.arange(N_DEV) == busiest, TILES_DEV, counts)
    return counts.astype(jnp.int32)


def block_scale(own_key, shape, cuts, low, high):
    level = 1.0
    for position, shards_of in cuts:
        steps = jax.random.uniform(jax.random.fold_in(jax.random.fold_in(own_key, 6), position), (shards_of,), jnp.float32, low / len(cuts), high / len(cuts))
        level = level * jnp.repeat(jnp.exp(steps), shape[position] // shards_of).reshape((-1,) + (1,) * (len(shape) - 1 - position))
    return level


def centred(own_key, dims, scale, most, split=(), kind=jnp.bfloat16):
    drawn = jax.random.normal(own_key, dims, jnp.float32) * scale
    if len(split) > 0:
        drawn = block_scale(own_key, dims, split, -0.22, 0.18) * drawn
    return jnp.clip(drawn, min=-most, max=most).astype(kind)


def setup_inputs(seed: int = 0) -> dict:
    splits = jax.random.split(jax.random.key(seed), 5)
    source = centred(splits[0], (FEAT, CELLS), 1.0, 6.0, ((1, 128),))
    weights = centred(splits[1], (TILES, BLK, BLK), (BLK * TILES_DEV // ACU_BLK_DEV) ** -0.5, 0.01953125, ((0, 128),))
    tile_map = draw_tile_map(jax.random.fold_in(splits[4], 71), 0)
    tile_count = draw_tile_count(jax.random.fold_in(splits[4], 71), 0)
    return dict(source=source, weights=weights, tile_map=tile_map, tile_count=tile_count)


def reference(source, weights, tile_map, tile_count):
    feat = source.shape[0]
    blocks = source.reshape(feat, N_DEV * SRC_BLK_DEV, BLK).astype(jnp.float32)

    def one_device(acc, device):
        start = device * TILES_DEV
        tile_w = lax.dynamic_slice_in_dim(weights, start, TILES_DEV, 0).astype(jnp.float32)
        mapped = lax.dynamic_slice_in_dim(tile_map, start, TILES_DEV, 1)
        block_ids = (device * SRC_BLK_DEV + mapped[0]).astype(jnp.int32)
        picked = jnp.take(blocks, block_ids, axis=1)
        product = jnp.einsum("ftc,tcn->tfn", picked, tile_w, precision=lax.Precision.HIGHEST)
        used = (jnp.arange(TILES_DEV, dtype=jnp.int32) < tile_count[device]).astype(jnp.float32)
        product = product * used[:, None, None]
        target = (mapped[1] * ACU_BLK_DEV + mapped[2]).astype(jnp.int32)
        return acc.at[target].add(product), None

    start_acc = jnp.zeros((N_DEV * ACU_BLK_DEV, feat, BLK), jnp.float32)
    acc, _ = lax.scan(one_device, start_acc, jnp.arange(N_DEV, dtype=jnp.int32))
    return jnp.transpose(acc, (1, 0, 2)).reshape(feat, N_DEV * ACU_BLK_DEV * BLK)
```

```python
import functools

import jax
import jax.numpy as jnp
from jax import lax
from jax.experimental import pallas as pl
from jax.experimental.pallas import tpu as pltpu
from jax.sharding import PartitionSpec as P

REACH = 4
LANES = 128
CHUNK = 64


def kernel(n, src_hbm, w_hbm, map_hbm, cnt_hbm, out_ref, w, src, log, map_v, map_s, cnt_s, idx_v, idx_s, send, recv,
           w_sem, in_sem, send_sem, recv_sem):
    tiles, blk = w.shape[0], w.shape[1]
    feat = src.shape[1]
    chunks = tiles // CHUNK
    groups = tiles // LANES
    own = lax.axis_index("dev")
    offsets = [d for d in range(-REACH, REACH + 1) if d != 0] + [n // 2]
    partners = [lax.rem(own + (d + n), n) for d in offsets]

    map_copy = pltpu.make_async_copy(map_hbm, map_v, in_sem.at[0])
    cnt_copy = pltpu.make_async_copy(cnt_hbm, cnt_s, in_sem.at[1])
    map_copy_s = pltpu.make_async_copy(map_hbm, map_s, in_sem.at[2])
    src_copy = pltpu.make_async_copy(src, src, in_sem.at[3])
    map_copy.start()
    cnt_copy.start()
    map_copy_s.start()

    @pl.loop(0, src.shape[0])
    def _(b):
        part = pl.ds(pl.multiple_of(b * blk, blk), blk)
        pltpu.make_async_copy(src_hbm.at[:, part], src.at[b], in_sem.at[3]).start()

    def w_copy(c):
        part = pl.ds(pl.multiple_of(c * CHUNK, CHUNK), CHUNK)
        return pltpu.make_async_copy(w_hbm.at[part], w.at[part], w_sem.at[c])

    @pl.loop(0, chunks)
    def _(c):
        w_copy(c).start()

    barrier = pltpu.get_barrier_semaphore()
    for partner in partners:
        pl.semaphore_signal(barrier, inc=1, device_id=(partner,), device_id_type=pl.DeviceIdType.MESH)

    map_copy.wait()
    cnt_copy.wait()
    lane = lax.broadcasted_iota(jnp.int32, (1, LANES), 1)
    row = lax.broadcasted_iota(jnp.int32, (LANES, LANES), 0)
    keys, columns = [], []
    for g in range(groups):
        up = map_v[1:2, g * LANES:(g + 1) * LANES] - own
        up = jnp.where(up < 0, up + n, up)
        key = jnp.where(up == n // 2, 2 * REACH + 1, jnp.where(up > n // 2, up - n, up) + REACH)
        key = jnp.where(lane + g * LANES < cnt_s[0], key, 2 * REACH + 2)
        keys.append(key)
        columns.append(jnp.transpose(jnp.broadcast_to(key, (LANES, LANES))))
    last = jnp.zeros((LANES, LANES), jnp.int32)
    for g in range(groups):
        prev = jnp.zeros((LANES, LANES), jnp.int32)
        for h in range(g):
            prev = jnp.where(columns[h] == keys[g], row + (h * LANES + 1), prev)
        here = jnp.logical_and(columns[g] == keys[g], row < lane)
        prev = jnp.where(here, row + (g * LANES + 1), prev)
        idx_v[g:g + 1, :] = jnp.max(prev, axis=0, keepdims=True)
        last = jnp.where(columns[g] == lane, row + (g * LANES + 1), last)
    idx_v[groups:groups + 1, :] = jnp.max(last, axis=0, keepdims=True)
    idx_copy = pltpu.make_async_copy(idx_v, idx_s, in_sem.at[4])
    idx_copy.start()
    log[0] = jnp.zeros((feat, blk), jnp.float32)
    map_copy_s.wait()
    src_copy.wait()
    idx_copy.wait()

    @pl.loop(0, chunks)
    def _(c):
        w_copy(c).wait()
        base = c * CHUNK
        group, rest = base // LANES, lax.rem(base, LANES)
        for u in range(0, CHUNK, 2):
            blocks = [map_s[0, base + u + v] for v in range(2)]
            lhs = jnp.concatenate(
                [src[b] for b in blocks], axis=0)
            rhs = jnp.concatenate([w[base + u], w[base + u + 1]], axis=1)
            both = jnp.dot(lhs, rhs, preferred_element_type=jnp.float32)
            for v in range(2):
                product = both[v * feat:(v + 1) * feat, v * blk:(v + 1) * blk]
                log[base + u + v + 1] = product + log[idx_s[group, rest + u + v]]

    for k in range(len(offsets)):
        slot = k if k < REACH else k + 1
        send[k] = log[idx_s[groups, slot]]
    pl.semaphore_wait(barrier, len(offsets))
    copies = []
    for k, partner in enumerate(partners):
        copies.append(pltpu.make_async_remote_copy(
            src_ref=send.at[k], dst_ref=recv.at[k], send_sem=send_sem.at[k], recv_sem=recv_sem.at[k],
            device_id=(partner,), device_id_type=pl.DeviceIdType.MESH))
        copies[-1].start()
    total = log[idx_s[groups, REACH]]
    for k in range(len(offsets)):
        copies[k].wait_recv()
        total = total + recv[k]
    out_ref[...] = total
    for k in range(len(offsets)):
        copies[k].wait_send()


def on_device(source, weights, tile_map, tile_count):
    n = lax.axis_size("dev")
    feat, cells = source.shape
    tiles, blk, _ = weights.shape
    partners = 2 * REACH + 1
    groups = tiles // LANES

    return pl.pallas_call(
        functools.partial(kernel, n),
        out_shape=jax.ShapeDtypeStruct((feat, blk), jnp.float32),
        in_specs=[pl.BlockSpec(memory_space=pl.ANY)] * 4,
        out_specs=pl.BlockSpec(memory_space=pltpu.VMEM),
        scratch_shapes=[
            pltpu.VMEM((tiles, blk, blk), jnp.bfloat16),
            pltpu.VMEM((cells // blk, feat, blk), jnp.bfloat16),
            pltpu.VMEM((tiles + 1, feat, blk), jnp.float32),
            pltpu.VMEM(tile_map.shape, jnp.int32),
            pltpu.SMEM(tile_map.shape, jnp.int32),
            pltpu.SMEM((1,), jnp.int32),
            pltpu.VMEM((8, LANES), jnp.int32),
            pltpu.SMEM((8, LANES), jnp.int32),
            pltpu.VMEM((partners, feat, blk), jnp.float32),
            pltpu.VMEM((partners, feat, blk), jnp.float32),
            pltpu.SemaphoreType.DMA((tiles // CHUNK,)),
            pltpu.SemaphoreType.DMA((5,)),
            pltpu.SemaphoreType.DMA((partners,)),
            pltpu.SemaphoreType.DMA((partners,)),
        ],
        compiler_params=pltpu.CompilerParams(
            collective_id=0, has_side_effects=True, vmem_limit_bytes=67043328),
        cost_estimate=pl.CostEstimate(
            flops=2 * tiles * feat * blk * blk, bytes_accessed=tiles * blk * blk * 2, transcendentals=0),
    )(source, weights, tile_map, tile_count)


def solution(mesh):
    return jax.shard_map(
        on_device,
        mesh=mesh,
        in_specs=(P(None, "dev"), P("dev", None, None), P(None, "dev"), P("dev")),
        out_specs=P(None, "dev"),
        check_vma=False,
    )
```

```python
import functools

import jax
import jax.numpy as jnp
from jax import lax
from jax.experimental import pallas as pl
from jax.experimental.pallas import tpu as pltpu
from jax.sharding import PartitionSpec as P

REACH = 4
LANES = 128
CHUNK = 64


def kernel(n, src_hbm, w_hbm, map_hbm, cnt_s, out_ref, w, src, log, map_v, map_s, idx_v, idx_s, send, recv,
           w_sem, in_sem, send_sem, recv_sem):
    tiles, blk = w.shape[0], w.shape[1]
    feat = src.shape[1]
    chunks = tiles // CHUNK
    groups = tiles // LANES
    own = lax.axis_index("dev")
    offsets = [d for d in range(-REACH, REACH + 1) if d != 0] + [n // 2]
    partners = [lax.rem(own + (d + n), n) for d in offsets]

    map_copy = pltpu.make_async_copy(map_hbm, map_v, in_sem.at[0])
    map_copy_s = pltpu.make_async_copy(map_hbm, map_s, in_sem.at[1])
    src_copy = pltpu.make_async_copy(src, src, in_sem.at[2])
    map_copy.start()
    map_copy_s.start()

    @pl.loop(0, src.shape[0])
    def _(b):
        part = pl.ds(pl.multiple_of(b * blk, blk), blk)
        pltpu.make_async_copy(src_hbm.at[:, part], src.at[b], in_sem.at[2]).start()

    def w_copy(c):
        part = pl.ds(pl.multiple_of(c * CHUNK, CHUNK), CHUNK)
        return pltpu.make_async_copy(w_hbm.at[part], w.at[part], w_sem.at[c])

    @pl.loop(0, chunks)
    def _(c):
        w_copy(c).start()

    barrier = pltpu.get_barrier_semaphore()
    for partner in partners:
        pl.semaphore_signal(barrier, inc=1, device_id=(partner,), device_id_type=pl.DeviceIdType.MESH)

    map_copy.wait()
    lane = lax.broadcasted_iota(jnp.int32, (1, LANES), 1)
    row = lax.broadcasted_iota(jnp.int32, (LANES, LANES), 0)
    keys, columns = [], []
    for g in range(groups):
        up = map_v[1:2, g * LANES:(g + 1) * LANES] - own
        up = jnp.where(up < 0, up + n, up)
        key = jnp.where(up == n // 2, 2 * REACH + 1, jnp.where(up > n // 2, up - n, up) + REACH)
        key = jnp.where(lane + g * LANES < cnt_s[0], key, 2 * REACH + 2)
        keys.append(key)
        columns.append(jnp.transpose(jnp.broadcast_to(key, (LANES, LANES))))
    last = jnp.zeros((LANES, LANES), jnp.int32)
    for g in range(groups):
        prev = jnp.zeros((LANES, LANES), jnp.int32)
        for h in range(g):
            prev = jnp.where(columns[h] == keys[g], row + (h * LANES + 1), prev)
        here = jnp.logical_and(columns[g] == keys[g], row < lane)
        prev = jnp.where(here, row + (g * LANES + 1), prev)
        idx_v[:, g * LANES:(g + 1) * LANES] = jnp.max(prev, axis=0, keepdims=True)
        last = jnp.where(columns[g] == lane, row + (g * LANES + 1), last)
    idx_v[:, tiles:tiles + LANES] = jnp.max(last, axis=0, keepdims=True)
    idx_copy = pltpu.make_async_copy(idx_v, idx_s, in_sem.at[3])
    idx_copy.start()
    log[0] = jnp.zeros((feat, blk), jnp.float32)
    map_copy_s.wait()
    src_copy.wait()
    idx_copy.wait()

    @pl.loop(0, chunks)
    def _(c):
        w_copy(c).wait()
        base = c * CHUNK
        for u in range(0, CHUNK, 2):
            blocks = [map_s[0, base + u + v] for v in range(2)]
            lhs = jnp.concatenate(
                [src[b] for b in blocks], axis=0)
            rhs = jnp.concatenate([w[base + u], w[base + u + 1]], axis=1)
            both = jnp.dot(lhs, rhs, preferred_element_type=jnp.float32)
            for v in range(2):
                product = both[v * feat:(v + 1) * feat, v * blk:(v + 1) * blk]
                log[base + u + v + 1] = product + log[idx_s[0, base + u + v]]

    for k in range(len(offsets)):
        slot = k if k < REACH else k + 1
        send[k] = log[idx_s[0, tiles + slot]]
    pl.semaphore_wait(barrier, len(offsets))
    def transfer(k, partner):
        return pltpu.make_async_remote_copy(
            src_ref=send.at[k], dst_ref=recv.at[k], send_sem=send_sem.at[k], recv_sem=recv_sem.at[k],
            device_id=(partner,), device_id_type=pl.DeviceIdType.MESH)

    place = lax.rem(own, 4)
    for turn in range(REACH):
        step = jnp.where(place == 3, (2, 1, 4, 3)[turn], jnp.where(place == 2, (3, 2, 4, 1)[turn], REACH - turn))
        transfer(step + (REACH - 1), lax.rem(own + step, n)).start()
    for k in range(REACH):
        transfer(k, partners[k]).start()
    transfer(2 * REACH, partners[2 * REACH]).start()
    total = log[idx_s[0, tiles + REACH]]
    for k in range(len(offsets)):
        transfer(k, partners[k]).wait_recv()
        total = total + recv[k]
    out_ref[...] = total
    for k in range(len(offsets)):
        transfer(k, partners[k]).wait_send()


def on_device(source, weights, tile_map, tile_count):
    n = lax.axis_size("dev")
    feat, cells = source.shape
    tiles, blk, _ = weights.shape
    partners = 2 * REACH + 1
    hbm = [pltpu.with_memory_space_constraint(x, pltpu.HBM) for x in (source, weights, tile_map)]

    return pl.pallas_call(
        functools.partial(kernel, n),
        out_shape=pltpu.VMEM((feat, blk), jnp.float32),
        in_specs=[pl.BlockSpec(memory_space=pltpu.HBM)] * 3 + [pl.BlockSpec(memory_space=pltpu.SMEM)],
        out_specs=pl.BlockSpec(memory_space=pltpu.VMEM),
        scratch_shapes=[
            pltpu.VMEM((tiles, blk, blk), jnp.bfloat16),
            pltpu.VMEM((cells // blk, feat, blk), jnp.bfloat16),
            pltpu.VMEM((tiles + 1, feat, blk), jnp.float32),
            pltpu.VMEM(tile_map.shape, jnp.int32),
            pltpu.SMEM(tile_map.shape, jnp.int32),
            pltpu.VMEM((1, tiles + LANES), jnp.int32),
            pltpu.SMEM((1, tiles + LANES), jnp.int32),
            pltpu.VMEM((partners, feat, blk), jnp.float32),
            pltpu.VMEM((partners, feat, blk), jnp.float32),
            pltpu.SemaphoreType.DMA((tiles // CHUNK,)),
            pltpu.SemaphoreType.DMA((4,)),
            pltpu.SemaphoreType.DMA((partners,)),
            pltpu.SemaphoreType.DMA((partners,)),
        ],
        compiler_params=pltpu.CompilerParams(
            collective_id=0, has_side_effects=True, vmem_limit_bytes=48 * 1024 * 1024),
        cost_estimate=pl.CostEstimate(
            flops=2 * tiles * feat * blk * blk, bytes_accessed=tiles * blk * blk * 2, transcendentals=0),
    )(*hbm, tile_count)


def solution(mesh):
    return jax.shard_map(
        on_device,
        mesh=mesh,
        in_specs=(P(None, "dev"), P("dev", None, None), P(None, "dev"), P("dev")),
        out_specs=P(None, "dev"),
        check_vma=False,
    )
```

```python
import functools

import jax
import jax.numpy as jnp
from jax import lax
from jax.experimental import pallas as pl
from jax.experimental.pallas import tpu as pltpu
from jax.sharding import PartitionSpec as P

REACH = 4
LANES = 128
CHUNK = 64


def kernel(n, src_hbm, w_hbm, map_hbm, cnt_s, out_ref, w, src_flat, src, log, map_v, map_s, idx_v, idx_s, send, recv,
           w_sem, in_sem, send_sem, recv_sem):
    tiles, blk = w.shape[0], w.shape[1]
    feat = src.shape[1]
    chunks = tiles // CHUNK
    groups = tiles // LANES
    own = lax.axis_index("dev")
    offsets = [d for d in range(-REACH, REACH + 1) if d != 0] + [n // 2]
    partners = [lax.rem(own + (d + n), n) for d in offsets]

    map_copy = pltpu.make_async_copy(map_hbm, map_v, in_sem.at[0])
    map_copy_s = pltpu.make_async_copy(map_hbm, map_s, in_sem.at[1])
    src_copy = pltpu.make_async_copy(src_hbm, src_flat, in_sem.at[2])
    map_copy.start()
    map_copy_s.start()

    src_copy.start()

    def w_copy(c):
        part = pl.ds(pl.multiple_of(c * CHUNK, CHUNK), CHUNK)
        return pltpu.make_async_copy(w_hbm.at[part], w.at[part], w_sem.at[c])

    @pl.loop(0, chunks)
    def _(c):
        w_copy(c).start()

    barrier = pltpu.get_barrier_semaphore()
    for partner in partners:
        pl.semaphore_signal(barrier, inc=1, device_id=(partner,), device_id_type=pl.DeviceIdType.MESH)

    map_copy.wait()
    lane = lax.broadcasted_iota(jnp.int32, (1, LANES), 1)
    row = lax.broadcasted_iota(jnp.int32, (LANES, LANES), 0)
    keys, columns = [], []
    for g in range(groups):
        up = map_v[1:2, g * LANES:(g + 1) * LANES] - own
        up = jnp.where(up < 0, up + n, up)
        key = jnp.where(up == n // 2, 2 * REACH + 1, jnp.where(up > n // 2, up - n, up) + REACH)
        key = jnp.where(lane + g * LANES < cnt_s[0], key, 2 * REACH + 2)
        keys.append(key)
        columns.append(jnp.transpose(jnp.broadcast_to(key, (LANES, LANES))))
    last = jnp.zeros((LANES, LANES), jnp.int32)
    for g in range(groups):
        prev = jnp.zeros((LANES, LANES), jnp.int32)
        for h in range(g):
            prev = jnp.where(columns[h] == keys[g], row + (h * LANES + 1), prev)
        here = jnp.logical_and(columns[g] == keys[g], row < lane)
        prev = jnp.where(here, row + (g * LANES + 1), prev)
        prev = jnp.max(prev, axis=0, keepdims=True)
        idx_v[:, g * LANES:(g + 1) * LANES] = jnp.where(lane + g * LANES < cnt_s[0], prev, 0)
        last = jnp.where(columns[g] == lane, row + (g * LANES + 1), last)
    idx_v[:, tiles:tiles + LANES] = jnp.max(last, axis=0, keepdims=True)
    idx_copy = pltpu.make_async_copy(idx_v, idx_s, in_sem.at[3])
    idx_copy.start()
    log[0] = jnp.zeros((feat, blk), jnp.float32)
    src_copy.wait()
    for b in range(src.shape[0]):
        src[b] = src_flat[:, b * blk:(b + 1) * blk]
    map_copy_s.wait()
    idx_copy.wait()

    @pl.loop(0, chunks)
    def _(c):
        w_copy(c).wait()
        base = c * CHUNK
        for u in range(0, CHUNK, 2):
            blocks = [map_s[0, base + u + v] for v in range(2)]
            lhs = jnp.concatenate(
                [src[b] for b in blocks], axis=0)
            rhs = jnp.concatenate([w[base + u], w[base + u + 1]], axis=1)
            both = jnp.dot(lhs, rhs, preferred_element_type=jnp.float32)
            for v in range(2):
                product = both[v * feat:(v + 1) * feat, v * blk:(v + 1) * blk]
                log[base + u + v + 1] = product + log[idx_s[0, base + u + v]]

    for k in range(len(offsets)):
        slot = k if k < REACH else k + 1
        send[k] = log[idx_s[0, tiles + slot]]
    pl.semaphore_wait(barrier, len(offsets))
    def transfer(k, partner):
        return pltpu.make_async_remote_copy(
            src_ref=send.at[k], dst_ref=recv.at[k], send_sem=send_sem.at[k], recv_sem=recv_sem.at[k],
            device_id=(partner,), device_id_type=pl.DeviceIdType.MESH)

    place = lax.rem(own, 4)
    for turn in range(REACH):
        step = jnp.where(place == 3, (2, 1, 4, 3)[turn], jnp.where(place == 2, (3, 2, 4, 1)[turn], REACH - turn))
        transfer(step + (REACH - 1), lax.rem(own + step, n)).start()
    for k in range(REACH):
        transfer(k, partners[k]).start()
    transfer(2 * REACH, partners[2 * REACH]).start()
    total = log[idx_s[0, tiles + REACH]]
    for k in range(len(offsets)):
        transfer(k, partners[k]).wait_recv()
        total = total + recv[k]
    out_ref[...] = total
    for k in range(len(offsets)):
        transfer(k, partners[k]).wait_send()


def on_device(source, weights, tile_map, tile_count):
    n = lax.axis_size("dev")
    feat, cells = source.shape
    tiles, blk, _ = weights.shape
    partners = 2 * REACH + 1
    hbm = [pltpu.with_memory_space_constraint(x, pltpu.HBM) for x in (source, weights, tile_map)]

    return pl.pallas_call(
        functools.partial(kernel, n),
        out_shape=pltpu.VMEM((feat, blk), jnp.float32),
        in_specs=[pl.BlockSpec(memory_space=pltpu.HBM)] * 3 + [pl.BlockSpec(memory_space=pltpu.SMEM)],
        out_specs=pl.BlockSpec(memory_space=pltpu.VMEM),
        scratch_shapes=[
            pltpu.VMEM((tiles, blk, blk), jnp.bfloat16),
            pltpu.VMEM((feat, cells), jnp.bfloat16),
            pltpu.VMEM((cells // blk, feat, blk), jnp.bfloat16),
            pltpu.VMEM((tiles + 1, feat, blk), jnp.float32),
            pltpu.VMEM(tile_map.shape, jnp.int32),
            pltpu.SMEM(tile_map.shape, jnp.int32),
            pltpu.VMEM((1, tiles + LANES), jnp.int32),
            pltpu.SMEM((1, tiles + LANES), jnp.int32),
            pltpu.VMEM((partners, feat, blk), jnp.float32),
            pltpu.VMEM((partners, feat, blk), jnp.float32),
            pltpu.SemaphoreType.DMA((tiles // CHUNK,)),
            pltpu.SemaphoreType.DMA((4,)),
            pltpu.SemaphoreType.DMA((partners,)),
            pltpu.SemaphoreType.DMA((partners,)),
        ],
        compiler_params=pltpu.CompilerParams(
            collective_id=0, has_side_effects=True, vmem_limit_bytes=48 * 1024 * 1024),
        cost_estimate=pl.CostEstimate(
            flops=2 * tiles * feat * blk * blk, bytes_accessed=tiles * blk * blk * 2, transcendentals=0),
    )(*hbm, tile_count)


def solution(mesh):
    return jax.shard_map(
        on_device,
        mesh=mesh,
        in_specs=(P(None, "dev"), P("dev", None, None), P(None, "dev"), P("dev")),
        out_specs=P(None, "dev"),
        check_vma=False,
    )
```

```python
import functools

import jax
import jax.numpy as jnp
from jax import lax
from jax.experimental import pallas as pl
from jax.experimental.pallas import tpu as pltpu
from jax.sharding import PartitionSpec as P

REACH = 4
LANES = 128
CHUNK = 64


def kernel(n, src_hbm, w_hbm, map_hbm, cnt_s, out_ref, w, src_flat, src, log, map_v, map_s, idx_v, idx_s, send, recv,
           w_sem, in_sem, send_sem, recv_sem):
    tiles, blk = w.shape[0], w.shape[1]
    feat = src.shape[1]
    chunks = tiles // CHUNK
    groups = tiles // LANES
    own = lax.axis_index("dev")
    offsets = [d for d in range(-REACH, REACH + 1) if d != 0] + [n // 2]
    partners = [lax.rem(own + (d + n), n) for d in offsets]

    map_copy = pltpu.make_async_copy(map_hbm, map_v, in_sem.at[0])
    map_copy_s = pltpu.make_async_copy(map_hbm, map_s, in_sem.at[1])
    src_copy = pltpu.make_async_copy(src_hbm, src_flat, in_sem.at[2])
    map_copy.start()
    map_copy_s.start()

    src_copy.start()

    def w_copy(c):
        part = pl.ds(pl.multiple_of(c * CHUNK, CHUNK), CHUNK)
        return pltpu.make_async_copy(w_hbm.at[part], w.at[part], w_sem.at[c])

    @pl.loop(0, chunks)
    def _(c):
        w_copy(c).start()

    barrier = pltpu.get_barrier_semaphore()
    for partner in partners:
        pl.semaphore_signal(barrier, inc=1, device_id=(partner,), device_id_type=pl.DeviceIdType.MESH)

    map_copy.wait()
    lane = lax.broadcasted_iota(jnp.int32, (1, LANES), 1)
    row = lax.broadcasted_iota(jnp.int32, (LANES, LANES), 0)
    keys, columns = [], []
    for g in range(groups):
        up = map_v[1:2, g * LANES:(g + 1) * LANES] - own
        up = jnp.where(up < 0, up + n, up)
        key = jnp.where(up == n // 2, 2 * REACH + 1, jnp.where(up > n // 2, up - n, up) + REACH)
        key = jnp.where(lane + g * LANES < cnt_s[0], key, 2 * REACH + 2)
        keys.append(key)
        columns.append(jnp.transpose(jnp.broadcast_to(key, (LANES, LANES))))
    last = jnp.zeros((LANES, LANES), jnp.int32)
    for g in range(groups):
        prev = jnp.zeros((LANES, LANES), jnp.int32)
        for h in range(g):
            prev = jnp.where(columns[h] == keys[g], row + (h * LANES + 1), prev)
        here = jnp.logical_and(columns[g] == keys[g], row < lane)
        prev = jnp.where(here, row + (g * LANES + 1), prev)
        prev = jnp.max(prev, axis=0, keepdims=True)
        idx_v[:, g * LANES:(g + 1) * LANES] = jnp.where(lane + g * LANES < cnt_s[0], prev, 0)
        last = jnp.where(columns[g] == lane, row + (g * LANES + 1), last)
    idx_v[:, tiles:tiles + LANES] = jnp.max(last, axis=0, keepdims=True)
    idx_copy = pltpu.make_async_copy(idx_v, idx_s, in_sem.at[3])
    idx_copy.start()
    log[0] = jnp.zeros((feat, blk), jnp.float32)
    src_copy.wait()
    for b in range(src.shape[0]):
        src[b] = src_flat[:, b * blk:(b + 1) * blk]
    map_copy_s.wait()
    idx_copy.wait()

    @pl.loop(0, chunks)
    def _(c):
        w_copy(c).wait()
        base = c * CHUNK
        for u in range(0, CHUNK, 2):
            blocks = [map_s[0, base + u + v] for v in range(2)]
            lhs = jnp.concatenate(
                [src[b] for b in blocks], axis=0)
            rhs = jnp.concatenate([w[base + u], w[base + u + 1]], axis=1)
            both = jnp.dot(lhs, rhs, preferred_element_type=jnp.float32)
            for v in range(2):
                product = both[v * feat:(v + 1) * feat, v * blk:(v + 1) * blk]
                log[base + u + v + 1] = product + log[idx_s[0, base + u + v]]

    for k in range(len(offsets)):
        slot = k if k < REACH else k + 1
        send[k] = log[idx_s[0, tiles + slot]]
    pl.semaphore_wait(barrier, len(offsets))
    def transfer(k, partner):
        return pltpu.make_async_remote_copy(
            src_ref=send.at[k], dst_ref=recv.at[k], send_sem=send_sem.at[k], recv_sem=recv_sem.at[k],
            device_id=(partner,), device_id_type=pl.DeviceIdType.MESH)

    place = lax.rem(own, 4)
    steps = [jnp.where(place == 3, (2, 1, 4, 3)[turn], jnp.where(place == 2, (3, 2, 4, 1)[turn], REACH - turn))
             for turn in range(REACH)]
    transfer(steps[0] + (REACH - 1), lax.rem(own + steps[0], n)).start()
    transfer(steps[1] + (REACH - 1), lax.rem(own + steps[1], n)).start()
    transfer(steps[2] + (REACH - 1), lax.rem(own + steps[2], n)).start()
    transfer(steps[3] + (REACH - 1), lax.rem(own + steps[3], n)).start()
    transfer(steps[0] + (REACH - 1), lax.rem(own + steps[0], n)).wait_send()
    transfer(steps[1] + (REACH - 1), lax.rem(own + steps[1], n)).wait_send()
    transfer(steps[2] + (REACH - 1), lax.rem(own + steps[2], n)).wait_send()
    transfer(steps[3] + (REACH - 1), lax.rem(own + steps[3], n)).wait_send()
    for k in range(REACH):
        transfer(k, partners[k]).start()
    transfer(2 * REACH, partners[2 * REACH]).start()
    total = log[idx_s[0, tiles + REACH]]
    for k in list(range(REACH)) + [2 * REACH, REACH, 2 * REACH - 1, REACH + 1, REACH + 2]:
        transfer(k, partners[k]).wait_recv()
        total = total + recv[k]
    out_ref[...] = total
    for k in list(range(REACH)) + [2 * REACH]:
        transfer(k, partners[k]).wait_send()


def on_device(source, weights, tile_map, tile_count):
    n = lax.axis_size("dev")
    feat, cells = source.shape
    tiles, blk, _ = weights.shape
    partners = 2 * REACH + 1
    hbm = [pltpu.with_memory_space_constraint(x, pltpu.HBM) for x in (source, weights, tile_map)]

    return pl.pallas_call(
        functools.partial(kernel, n),
        out_shape=pltpu.VMEM((feat, blk), jnp.float32),
        in_specs=[pl.BlockSpec(memory_space=pltpu.HBM)] * 3 + [pl.BlockSpec(memory_space=pltpu.SMEM)],
        out_specs=pl.BlockSpec(memory_space=pltpu.VMEM),
        scratch_shapes=[
            pltpu.VMEM((tiles, blk, blk), jnp.bfloat16),
            pltpu.VMEM((feat, cells), jnp.bfloat16),
            pltpu.VMEM((cells // blk, feat, blk), jnp.bfloat16),
            pltpu.VMEM((tiles + 1, feat, blk), jnp.float32),
            pltpu.VMEM(tile_map.shape, jnp.int32),
            pltpu.SMEM(tile_map.shape, jnp.int32),
            pltpu.VMEM((1, tiles + LANES), jnp.int32),
            pltpu.SMEM((1, tiles + LANES), jnp.int32),
            pltpu.VMEM((partners, feat, blk), jnp.float32),
            pltpu.VMEM((partners, feat, blk), jnp.float32),
            pltpu.SemaphoreType.DMA((tiles // CHUNK,)),
            pltpu.SemaphoreType.DMA((4,)),
            pltpu.SemaphoreType.DMA((partners,)),
            pltpu.SemaphoreType.DMA((partners,)),
        ],
        compiler_params=pltpu.CompilerParams(
            collective_id=0, has_side_effects=True, vmem_limit_bytes=48 * 1024 * 1024),
        cost_estimate=pl.CostEstimate(
            flops=2 * tiles * feat * blk * blk, bytes_accessed=tiles * blk * blk * 2, transcendentals=0),
    )(*hbm, tile_count)


def solution(mesh):
    return jax.shard_map(
        on_device,
        mesh=mesh,
        in_specs=(P(None, "dev"), P("dev", None, None), P(None, "dev"), P("dev")),
        out_specs=P(None, "dev"),
        check_vma=False,
    )
```
